32 devices in a mesh: groups: 2 (over y), expert: 16 (over z, x, core).
Axes of the slice: x: 2, y: 2, z: 4, core: 2. Of those that a mesh axis runs over, the one named last changes fastest.
Arguments:
- tokens: bfloat16 [512, 3584], P(('groups', 'expert')), parts along dimension 0, may hold values from -6 to 6
- live_counts: int32 [32], P(('groups', 'expert')), parts along dimension 0, may hold values from 8 to 16, as said below
- expert_ids: int32 [512, 4], P(('groups', 'expert')), parts along dimension 0, may hold values from 0 to 7, all different within a row; in each aligned block of 16 rows (0 to 15, 16 to 31, ...) at most 16 rows name the same one
- gate_scores: float32 [512, 4], P(('groups', 'expert')), parts along dimension 0, may hold values from 0.1 to 1
- gate_weight: bfloat16 [16, 3584, 512], P('expert'), may hold values from -0.09375 to 0.09375
- up_weight: bfloat16 [16, 3584, 512], P('expert'), may hold values from -0.09375 to 0.09375
- down_weight: bfloat16 [16, 512, 3584], P('expert'), may hold values from -0.1875 to 0.1875
Outputs:
- moe_out: bfloat16 [512, 3584], P(('groups', 'expert')), parts along dimension 0
The draws below stay inside these ranges and needn't reach their ends.
There are 2 independent parts, one for each index of `groups`. The reference program is written for one: setup_inputs(seed, part) draws one part's arguments, and reference() takes and returns one part's arrays. A program takes and returns all parts, laid end to end along the dimension named above; an argument that names none is the same for every part. Nothing has to cross between parts.
Inputs may be any that keep to these rules, and one draw needn't show every extreme that they name: `expert_ids`: A row names 4 different experts. In each device's aligned block of 16 rows no expert is named by more than 16 rows, a bound that some block reaches. `live_counts`: some device has all 16 slots live.
All inputs are finite; a program needn't handle non-finite values.
Results may differ from the reference program's by a relative error of at most 0.0068.
Values may be sent and summed in bfloat16 or wider, within the bound.
No kernel may reach another device: no remote copies, remote signals or barrier semaphores. Data moves between devices by JAX's collectives and lax.ppermute only.
A program may use at most 64 MiB of HBM per device.

```python
import math
import jax
import jax.numpy as jnp
import numpy as np
from jax import lax

D = 3584
FF = 1024
TOP = 4
TOK_DEV = 16
FF_HALF = 512
EXPERTS = 8
CAP = 16
TOKENS = 256
N_EXPERT = 16


def draw_live_counts(key, part):
    devices = TOKENS // TOK_DEV
    counts = jax.random.randint(jax.random.fold_in(key, 11), (devices,), TOK_DEV // 2, TOK_DEV + 1)
    full_device = jax.random.randint(jax.random.fold_in(key, 12), (), 0, devices)
    counts = jnp.where(jnp.arange(devices) == full_device, TOK_DEV, counts)
    return counts.astype(jnp.int32)


def block_scale(key, extent, pieces, least, largest):
    level, own = 1.0, jax.random.fold_in(key, 6)
    for dim, shards_of in pieces:
        heights = jnp.exp(jax.random.uniform(jax.random.fold_in(own, dim), (shards_of,), jnp.float32, least / len(pieces), largest / len(pieces)))
        level = level * jnp.repeat(heights, extent[dim] // shards_of).reshape([-1 if axis == dim else 1 for axis in range(len(extent))])
    return level


def shared_out(rng, own, number, rows, amount, top, most, slope):
    order = jax.random.permutation(rng, amount)
    packed, usual = portions_of(amount, rows * top, most, slope, True), portions_of(amount, rows * top, most, slope, False)
    places = jnp.arange(amount)

    def named(sizes, turn):
        used = int((sizes > 0).sum())
        fixed = max(1, used // 4)
        passed = fixed + (places - fixed + turn * (used - fixed)) % max(1, amount - fixed)
        return jnp.zeros((amount,), jnp.int32).at[order[jnp.where(places < fixed, places, passed)]].set(jnp.asarray(sizes, jnp.int32))

    sizes = jnp.where(number % 4 == 0, named(packed, number // 4), named(usual, number - number // 4 - 1))
    mixed = jax.random.permutation(jax.random.fold_in(own, 3), amount)
    giver, receiver = mixed[0:amount // 2 * 2:2], mixed[1:amount // 2 * 2:2]
    margin = jnp.minimum(sizes[giver] - 1, most - sizes[receiver]) // 2
    margin = jnp.where((giver == order[0]) | (receiver == order[0]) | (sizes[receiver] == 0), 0, jnp.maximum(margin, 0))
    passed = jax.random.randint(jax.random.fold_in(own, 4), (amount // 2,), 0, 1 << 20) % (margin + 1)
    sizes = sizes.at[giver].add(-passed).at[receiver].add(passed)
    items = jnp.searchsorted(jnp.cumsum(sizes), jnp.arange(rows * top), side="right").astype(jnp.int32)
    table = items.reshape(top, rows).T
    table = table[jax.random.permutation(jax.random.fold_in(own, 1), rows)]
    turn = jax.random.randint(jax.random.fold_in(own, 2), (rows, 1), 0, top)
    return jnp.take_along_axis(table, (jnp.arange(top)[None, :] + turn) % top, axis=1)


def portions_of(number_of, total, most, lean, full):
    portions = [(1 << 20) // math.isqrt(standing ** lean) + 1 for standing in range(1, number_of + 1)]
    largest = most if full else min(most, max(-(-total // number_of), total * portions[0] // sum(portions)))
    least = 1 if total - largest >= number_of - 1 else 0
    given, surplus = [largest] + [least] * (number_of - 1), total - largest - least * (number_of - 1)
    while surplus > 0:
        candidates = [i for i in range(1, number_of) if given[i] < largest] or [i for i in range(1, number_of) if given[i] < most]
        pool, left = sum([portions[i] for i in candidates]), surplus
        for i in candidates:
            addition = min(most - given[i], max(1, left * portions[i] // pool), surplus)
            given[i] = given[i] + addition
            surplus = surplus - addition
    return np.array(given)


def noise(own_key, extent, width, limit, pieces=(), kind=jnp.bfloat16):
    gain = block_scale(own_key, extent, pieces, -0.22, 0.18) if pieces else 1.0
    result = jax.random.normal(own_key, extent, jnp.float32) * width * gain
    return jnp.minimum(jnp.maximum(result, -limit), limit).astype(kind)


def setup_inputs(seed: int = 0, part: int = 0) -> dict:
    key_list = jax.random.split(jax.random.key(seed), 8)
    part_splits = jax.random.split(jax.random.fold_in(key_list[7], part), 8)
    tokens = noise(part_splits[0], (TOKENS, D), 1.0, 6.0, ((0, 16),))
    live_counts = draw_live_counts(jax.random.fold_in(jax.random.fold_in(key_list[7], part), 71), part)
    expert_ids_keys = jax.random.split(jax.random.fold_in(part_splits[2], 1), TOKENS // TOK_DEV)
    expert_ids_turns = jax.random.permutation(jax.random.fold_in(part_splits[2], 3), TOKENS // TOK_DEV)
    expert_ids = jax.vmap(lambda own, number: shared_out(jax.random.fold_in(part_splits[2], 2), own, number, TOK_DEV, EXPERTS, TOP, CAP, 2))(expert_ids_keys, expert_ids_turns).reshape((TOKENS, TOP))
    gate_scores = jnp.clip(jnp.exp(math.log(1.0) - 2.3025851 * jax.random.uniform(part_splits[3], (TOKENS, TOP), jnp.float32) ** block_scale(part_splits[3], (TOKENS, TOP), ((0, 16),), -0.2, 0.2)), 0.1, 1.0)
    gate_weight = noise(key_list[4], (N_EXPERT, D, FF_HALF), D ** -0.5, 0.09375, ((0, 16),))
    up_weight = noise(key_list[5], (N_EXPERT, D, FF_HALF), D ** -0.5, 0.09375, ((0, 16),))
    down_weight = noise(key_list[6], (N_EXPERT, FF_HALF, D), FF ** -0.5, 0.1875, ((0, 16),))
    return dict(tokens=tokens, live_counts=live_counts, expert_ids=expert_ids, gate_scores=gate_scores, gate_weight=gate_weight, up_weight=up_weight, down_weight=down_weight)


def expert_rows(gate_pair, up_pair, down_pair, inputs):
    gate_full = jnp.concatenate([gate_pair[0], gate_pair[1]], axis=1)
    up_full = jnp.concatenate([up_pair[0], up_pair[1]], axis=1)
    down_full = jnp.concatenate([down_pair[0], down_pair[1]], axis=0)
    gate_act = jnp.dot(inputs, gate_full, preferred_element_type=jnp.float32)
    up_act = jnp.dot(inputs, up_full, preferred_element_type=jnp.float32)
    hidden = (jax.nn.silu(gate_act) * up_act).astype(jnp.bfloat16)
    return jnp.dot(hidden, down_full, preferred_element_type=jnp.float32).astype(jnp.bfloat16)


def reference(tokens, live_counts, expert_ids, gate_scores, gate_weight, up_weight, down_weight):
    devices = N_EXPERT
    block_ids = expert_ids.reshape(devices, TOK_DEV * TOP)
    onehot = (block_ids[:, :, None] == jnp.arange(EXPERTS, dtype=jnp.int32)[None, None, :]).astype(jnp.int32)
    earlier = jnp.cumsum(onehot, axis=1) - onehot
    slot_index = jnp.sum(earlier * onehot, axis=2)
    source = jnp.arange(devices, dtype=jnp.int32)[:, None]
    position = (source * CAP + slot_index).reshape(-1).astype(jnp.int32)
    token_index = jnp.repeat(jnp.arange(TOKENS, dtype=jnp.int32), TOP)
    flat_ids = expert_ids.reshape(-1).astype(jnp.int32)
    slot_table = jnp.full((EXPERTS, devices * CAP), TOKENS, dtype=jnp.int32)
    slot_table = slot_table.at[flat_ids, position].set(token_index)
    padded = jnp.concatenate([tokens, jnp.zeros((1, D), tokens.dtype)], axis=0)

    def one_expert(items):
        gate_pair, up_pair, down_pair, table_row = items
        return expert_rows(gate_pair, up_pair, down_pair, padded[table_row])

    results = lax.map(one_expert, (gate_weight.reshape(EXPERTS, 2, D, FF_HALF),
                                   up_weight.reshape(EXPERTS, 2, D, FF_HALF),
                                   down_weight.reshape(EXPERTS, 2, FF_HALF, D),
                                   slot_table))
    picked = results[flat_ids, position].reshape(TOKENS, TOP, D).astype(jnp.float32)
    weighted = jnp.sum(picked * gate_scores[:, :, None].astype(jnp.float32), axis=1)
    local_pos = jnp.arange(TOKENS, dtype=jnp.int32) % TOK_DEV
    live_mask = local_pos < jnp.repeat(live_counts, TOK_DEV)
    return jnp.where(live_mask[:, None], weighted, jnp.zeros_like(weighted)).astype(jnp.bfloat16)
```

```python
import jax
import jax.numpy as jnp
from jax import lax
from jax.sharding import PartitionSpec as P

LANES = 128


def stage_bits(count):
    top = count.bit_length() - 1
    even = list(range(top - 1, 0, -1))
    odd = even[-1:] + even[:-1]
    return list(zip(even, odd))


def swap(block, bits):
    count = lax.axis_size("expert")
    route = [(i, i ^ (1 << bits[i & 1])) for i in range(count)]
    return lax.ppermute(block, "expert", route)


def gather_rows(rows, count):
    for bits in stage_bits(count):
        rows = jnp.concatenate([rows, swap(rows, bits)], axis=0)
    return rows


def reduce_rows(part, count):
    for bits in stage_bits(count)[::-1]:
        half = part.shape[0] // 2
        got = swap(part[half:].astype(jnp.bfloat16), bits)
        part = part[:half] + got.astype(jnp.float32)
    return part


def routing_columns(live_counts, expert_ids, gate_scores, experts):
    slots = expert_ids.shape[0]
    live = jnp.arange(slots, dtype=jnp.int32)[:, None] < live_counts[0]
    named = expert_ids[:, :, None] == jnp.arange(experts, dtype=jnp.int32)
    score = jnp.sum(jnp.where(named & live[:, :, None], gate_scores[:, :, None], 0.0), axis=1)
    high = lax.reduce_precision(score, 8, 7)
    low = score - high
    pad = jnp.zeros((slots, -2 * experts % LANES), jnp.float32)
    return jnp.concatenate([high, low, pad], axis=1).astype(jnp.bfloat16)


def hidden_rows(rows, width, mine, experts, gate_weight, up_weight):
    inputs, columns = rows[:, :width], rows[:, width:]
    lane = jnp.arange(columns.shape[1], dtype=jnp.int32)
    own = (lane < 2 * experts) & (lane % experts == mine)
    score = jnp.sum(jnp.where(own, columns.astype(jnp.float32), 0.0), axis=1, keepdims=True)
    gate_act = jnp.dot(inputs, gate_weight[0], preferred_element_type=jnp.float32)
    up_act = jnp.dot(inputs, up_weight[0], preferred_element_type=jnp.float32)
    return (jax.nn.silu(gate_act) * up_act).astype(jnp.bfloat16), score


def shards(tokens, live_counts, expert_ids, gate_scores, gate_weight, up_weight, down_weight):
    width = tokens.shape[1]
    count = lax.axis_size("expert")
    experts = count // 2
    mine = lax.shift_right_logical(lax.axis_index("expert"), 1)
    columns = routing_columns(live_counts, expert_ids, gate_scores, experts)
    near = gather_rows(jnp.concatenate([tokens, columns], axis=1), count)
    far = swap(near, (0, 0))
    near_hidden, near_score = hidden_rows(near, width, mine, experts, gate_weight, up_weight)
    far_hidden, far_score = hidden_rows(far, width, mine, experts, gate_weight, up_weight)
    far_part = jnp.dot(far_hidden, down_weight[0], preferred_element_type=jnp.float32) * far_score
    got = swap(far_part.astype(jnp.bfloat16), (0, 0))
    near_part = jnp.dot(near_hidden, down_weight[0], preferred_element_type=jnp.float32) * near_score
    part = near_part + got.astype(jnp.float32)
    return reduce_rows(part, count).astype(jnp.bfloat16)


def solution(mesh):
    in_specs = (
        P(("groups", "expert"), None),
        P(("groups", "expert")),
        P(("groups", "expert"), None),
        P(("groups", "expert"), None),
        P("expert", None, None),
        P("expert", None, None),
        P("expert", None, None),
    )
    out_specs = P(("groups", "expert"), None)
    return jax.shard_map(shards, mesh=mesh, in_specs=in_specs, out_specs=out_specs, check_vma=False)
```

```python
import jax
import jax.numpy as jnp
from jax import lax
from jax.experimental import pallas as pl
from jax.experimental.pallas import tpu as pltpu
from jax.sharding import PartitionSpec as P

LANES = 128


def stage_bits(count):
    top = count.bit_length() - 1
    even = list(range(top - 1, 0, -1))
    odd = even[-1:] + even[:-1]
    return list(zip(even, odd))


def swap(block, bits):
    count = lax.axis_size("expert")
    route = [(i, i ^ (1 << bits[i & 1])) for i in range(count)]
    return lax.ppermute(block, "expert", route)


def gather_rows(rows, count):
    for bits in stage_bits(count):
        rows = jnp.concatenate([rows, swap(rows, bits)], axis=0)
    return rows


def reduce_rows(part, count):
    for bits in stage_bits(count)[::-1]:
        half = part.shape[0] // 2
        got = swap(part[half:].astype(jnp.bfloat16), bits)
        part = part[:half] + got.astype(jnp.float32)
    return part


def routing_columns(live_counts, expert_ids, gate_scores, experts):
    slots = expert_ids.shape[0]
    live = jnp.arange(slots, dtype=jnp.int32)[:, None] < live_counts[0]
    named = expert_ids[:, :, None] == jnp.arange(experts, dtype=jnp.int32)
    score = jnp.sum(jnp.where(named & live[:, :, None], gate_scores[:, :, None], 0.0), axis=1)
    high = lax.reduce_precision(score, 8, 7)
    low = score - high
    pad = jnp.zeros((slots, -2 * experts % LANES), jnp.float32)
    return jnp.concatenate([high, low, pad], axis=1).astype(jnp.bfloat16)


def expert_body(rows, score, gate_a, up_a, down_a, gate_b, up_b, down_b, out):
    step, steps = pl.program_id(1), pl.num_programs(1)
    inputs = rows[:, : out.shape[1]]

    def add_units(gate, up, down):
        gate_act = jnp.dot(inputs, gate[0], preferred_element_type=jnp.float32)
        up_act = jnp.dot(inputs, up[0], preferred_element_type=jnp.float32)
        hidden = (gate_act / (1.0 + jnp.exp(-gate_act)) * up_act).astype(jnp.bfloat16)
        return jnp.dot(hidden, down[0], preferred_element_type=jnp.float32)

    @pl.when(step == 0)
    def _():
        out[...] = add_units(gate_a, up_a, down_a)

    @pl.when((step > 0) & (step < steps // 2))
    def _():
        out[...] += add_units(gate_a, up_a, down_a)

    @pl.when((step >= steps // 2) & (step < steps - 1))
    def _():
        out[...] += add_units(gate_b, up_b, down_b)

    @pl.when(step == steps - 1)
    def _():
        out[...] = (out[...] + add_units(gate_b, up_b, down_b)) * score[...]


def expert_rows(rows, score, own, other):
    count, units, width = rows.shape[0], own[2].shape[1], own[2].shape[2]
    tile = min(count, 256)
    block = min(units, 256)
    half = units // block

    def first(j):
        return jnp.minimum(j, half - 1)

    def second(j):
        return jnp.maximum(j - half, 0)

    def specs(at):
        side = pl.BlockSpec((1, width, block), lambda i, j: (0, 0, at(j)))
        return [side, side, pl.BlockSpec((1, block, width), lambda i, j: (0, at(j), 0))]

    return pl.pallas_call(
        expert_body,
        grid=(count // tile, 2 * half),
        in_specs=[
            pl.BlockSpec((tile, rows.shape[1]), lambda i, j: (i, 0)),
            pl.BlockSpec((tile, 1), lambda i, j: (i, 0)),
        ]
        + specs(first)
        + specs(second),
        out_specs=pl.BlockSpec((tile, width), lambda i, j: (i, 0)),
        out_shape=jax.ShapeDtypeStruct((count, width), jnp.float32),
        compiler_params=pltpu.CompilerParams(
            dimension_semantics=("arbitrary", "arbitrary"), vmem_limit_bytes=50 * 2**20
        ),
        cost_estimate=pl.CostEstimate(
            flops=12 * count * units * width, bytes_accessed=12 * units * width, transcendentals=0
        ),
        name="experts",
    )(rows, score, *own, *other)


def shards(tokens, live_counts, expert_ids, gate_scores, gate_weight, up_weight, down_weight):
    width = tokens.shape[1]
    count = lax.axis_size("expert")
    experts = count // 2
    mine = lax.shift_right_logical(lax.axis_index("expert"), 1)
    own = (gate_weight, up_weight, down_weight)
    other = [swap(weight, (0, 0)) for weight in own]
    columns = routing_columns(live_counts, expert_ids, gate_scores, experts)
    rows = gather_rows(jnp.concatenate([tokens, columns], axis=1), count)
    columns = rows[:, width:]
    lane = jnp.arange(columns.shape[1], dtype=jnp.int32)
    named = (lane < 2 * experts) & (lane % experts == mine)
    score = jnp.sum(jnp.where(named, columns.astype(jnp.float32), 0.0), axis=1, keepdims=True)
    part = expert_rows(rows, score, own, other)
    return reduce_rows(part, count).astype(jnp.bfloat16)


def solution(mesh):
    in_specs = (
        P(("groups", "expert"), None),
        P(("groups", "expert")),
        P(("groups", "expert"), None),
        P(("groups", "expert"), None),
        P("expert", None, None),
        P("expert", None, None),
        P("expert", None, None),
    )
    out_specs = P(("groups", "expert"), None)
    return jax.shard_map(shards, mesh=mesh, in_specs=in_specs, out_specs=out_specs, check_vma=False)
```

```python
import jax
import jax.numpy as jnp
from jax import lax
from jax.experimental import pallas as pl
from jax.experimental.pallas import tpu as pltpu
from jax.sharding import PartitionSpec as P

LANES = 128


def stage_bits(count):
    top = count.bit_length() - 1
    even = list(range(top - 1, 0, -1))
    odd = even[-1:] + even[:-1]
    return list(zip(even, odd))


def swap(block, bits):
    count = lax.axis_size("expert")
    route = [(i, i ^ (1 << bits[i & 1])) for i in range(count)]
    return lax.ppermute(block, "expert", route)


def gather_rows(rows, stages):
    for bits in stages:
        rows = jnp.concatenate([rows, swap(rows, bits)], axis=0)
    return rows


def reduce_rows(part, count):
    for bits in stage_bits(count)[::-1]:
        half = part.shape[0] // 2
        got = swap(part[half:].astype(jnp.bfloat16), bits)
        part = part[:half] + got.astype(jnp.float32)
    return part


def routing_columns(live_counts, expert_ids, gate_scores, experts):
    slots = expert_ids.shape[0]
    live = jnp.arange(slots, dtype=jnp.int32)[:, None] < live_counts[0]
    named = expert_ids[:, :, None] == jnp.arange(experts, dtype=jnp.int32)
    score = jnp.sum(jnp.where(named & live[:, :, None], gate_scores[:, :, None], 0.0), axis=1)
    high = lax.reduce_precision(score, 8, 7)
    low = score - high
    pad = jnp.zeros((slots, -2 * experts % LANES), jnp.float32)
    return jnp.concatenate([high, low, pad], axis=1).astype(jnp.bfloat16)


def load_body(*refs):
    half = len(refs) // 2
    sources, targets, sems = refs[:half], refs[half:-1], refs[-1]
    copies = [
        pltpu.make_async_copy(source, target, sems.at[i])
        for i, (source, target) in enumerate(zip(sources, targets))
    ]
    for copy in copies:
        copy.start()
    for copy in copies:
        copy.wait()


def load_weights(weights):
    return pl.pallas_call(
        load_body,
        in_specs=[pl.BlockSpec(memory_space=pltpu.HBM)] * len(weights),
        out_specs=[pl.BlockSpec(memory_space=pltpu.VMEM)] * len(weights),
        out_shape=[pltpu.VMEM(w.shape, w.dtype) for w in weights],
        scratch_shapes=[pltpu.SemaphoreType.DMA((len(weights),))],
        cost_estimate=pl.CostEstimate(
            flops=10**10, bytes_accessed=2 * sum(w.size for w in weights), transcendentals=0
        ),
        compiler_params=pltpu.CompilerParams(vmem_limit_bytes=2**20),
        name="load",
    )(*weights)


def expert_body(rows, gate_a, up_a, down_a, gate_b, up_b, down_b, out):
    width = out.shape[1]
    inputs = rows[:, :width]
    columns = rows[:, width:].astype(jnp.float32)
    experts = lax.axis_size("expert") // 2
    mine = lax.shift_right_logical(lax.axis_index("expert"), 1)
    lane = lax.broadcasted_iota(jnp.int32, columns.shape, 1)
    named = (lane == mine) | (lane == mine + experts)
    score = jnp.sum(jnp.where(named, columns, 0.0), axis=1, keepdims=True)

    def hidden(gate, up):
        gate_act = jnp.dot(inputs, gate[0], preferred_element_type=jnp.float32)
        up_act = jnp.dot(inputs, up[0], preferred_element_type=jnp.float32)
        return (gate_act / (1.0 + jnp.exp(-gate_act)) * up_act).astype(jnp.bfloat16)

    hidden_a, hidden_b = hidden(gate_a, up_a), hidden(gate_b, up_b)
    step = 512 if width % 512 == 0 else LANES
    for at in range(0, width, step):
        cols = slice(at, at + step)
        value = jnp.dot(hidden_a, down_a[0, :, cols], preferred_element_type=jnp.float32)
        value += jnp.dot(hidden_b, down_b[0, :, cols], preferred_element_type=jnp.float32)
        out[:, cols] = value * score


def expert_rows(rows, weights):
    count, width = rows.shape[0], weights[2].shape[2]
    tile = min(count, 256)
    return pl.pallas_call(
        expert_body,
        grid=(count // tile,),
        in_specs=[
            pl.BlockSpec((tile, rows.shape[1]), lambda i: (i, 0)),
        ]
        + [pl.BlockSpec(memory_space=pltpu.VMEM)] * len(weights),
        out_specs=pl.BlockSpec((tile, width), lambda i: (i, 0)),
        out_shape=jax.ShapeDtypeStruct((count, width), jnp.float32),
        compiler_params=pltpu.CompilerParams(
            dimension_semantics=("arbitrary",), vmem_limit_bytes=24 * 2**20
        ),
        name="experts",
    )(rows, *weights)


def shards(tokens, live_counts, expert_ids, gate_scores, gate_weight, up_weight, down_weight):
    count = lax.axis_size("expert")
    experts = count // 2
    own = (gate_weight, up_weight, down_weight)
    other = [swap(weight, (0, 0)) for weight in own]
    columns = routing_columns(live_counts, expert_ids, gate_scores, experts)
    rows = jnp.concatenate([tokens, columns], axis=1)
    stages = stage_bits(count)
    rows = gather_rows(rows, stages[:-1])
    rows, other = lax.optimization_barrier((rows, other))
    weights = load_weights([*own, *other])
    rows = gather_rows(rows, stages[-1:])
    part = expert_rows(rows, weights)
    return reduce_rows(part, count).astype(jnp.bfloat16)


def solution(mesh):
    in_specs = (
        P(("groups", "expert"), None),
        P(("groups", "expert")),
        P(("groups", "expert"), None),
        P(("groups", "expert"), None),
        P("expert", None, None),
        P("expert", None, None),
        P("expert", None, None),
    )
    out_specs = P(("groups", "expert"), None)
    return jax.shard_map(shards, mesh=mesh, in_specs=in_specs, out_specs=out_specs, check_vma=False)
```

```python
import jax
import jax.numpy as jnp
from jax import lax
from jax.experimental import pallas as pl
from jax.experimental.pallas import tpu as pltpu
from jax.sharding import PartitionSpec as P

LANES = 128


def stage_bits(count):
    top = count.bit_length() - 1
    even = list(range(top - 1, 0, -1))
    odd = even[-1:] + even[:-1]
    return list(zip(even, odd))


def swap(block, bits):
    count = lax.axis_size("expert")
    route = [(i, i ^ (1 << bits[i & 1])) for i in range(count)]
    return lax.ppermute(block, "expert", route)


def gather_rows(rows, stages):
    for bits in stages:
        rows = jnp.concatenate([rows, swap(rows, bits)], axis=0)
    return rows


def reduce_rows(part, count):
    for bits in stage_bits(count)[::-1]:
        half = part.shape[0] // 2
        got = swap(part[half:].astype(jnp.bfloat16), bits)
        part = part[:half] + got.astype(jnp.float32)
    return part


def routing_columns(live_counts, expert_ids, gate_scores, experts):
    slots = expert_ids.shape[0]
    live = jnp.arange(slots, dtype=jnp.int32)[:, None] < live_counts[0]
    named = expert_ids[:, :, None] == jnp.arange(experts, dtype=jnp.int32)
    score = jnp.sum(jnp.where(named & live[:, :, None], gate_scores[:, :, None], 0.0), axis=1)
    high = lax.reduce_precision(score, 8, 7)
    low = score - high
    pad = jnp.zeros((slots, -2 * experts % LANES), jnp.float32)
    return jnp.concatenate([high, low, pad], axis=1).astype(jnp.bfloat16)


def load_body(*refs):
    half = len(refs) // 2
    sources, targets, sems = refs[:half], refs[half:-1], refs[-1]
    copies = [
        pltpu.make_async_copy(source, target, sems.at[i])
        for i, (source, target) in enumerate(zip(sources, targets))
    ]
    for copy in copies:
        copy.start()
    for copy in copies:
        copy.wait()


def load_weights(weights):
    return pl.pallas_call(
        load_body,
        in_specs=[pl.BlockSpec(memory_space=pltpu.HBM)] * len(weights),
        out_specs=[pl.BlockSpec(memory_space=pltpu.VMEM)] * len(weights),
        out_shape=[pltpu.VMEM(w.shape, w.dtype) for w in weights],
        scratch_shapes=[pltpu.SemaphoreType.DMA((len(weights),))],
        cost_estimate=pl.CostEstimate(
            flops=10**10, bytes_accessed=0, transcendentals=0
        ),
        compiler_params=pltpu.CompilerParams(vmem_limit_bytes=2**20),
        name="load",
    )(*weights)


def expert_body(rows, gate_a, up_a, down_a, gate_b, up_b, down_b, out):
    width = out.shape[1]
    inputs = rows[:, :width]
    columns = rows[:, width:].astype(jnp.float32)
    experts = lax.axis_size("expert") // 2
    mine = lax.shift_right_logical(lax.axis_index("expert"), 1)
    lane = lax.broadcasted_iota(jnp.int32, columns.shape, 1)
    named = (lane == mine) | (lane == mine + experts)
    score = jnp.sum(jnp.where(named, columns, 0.0), axis=1, keepdims=True)

    def hidden(gate, up):
        gate_act = jnp.dot(inputs, gate[0], preferred_element_type=jnp.float32)
        up_act = jnp.dot(inputs, up[0], preferred_element_type=jnp.float32)
        return (gate_act / (1.0 + jnp.exp(-gate_act)) * up_act).astype(jnp.bfloat16)

    hidden_a, hidden_b = hidden(gate_a, up_a), hidden(gate_b, up_b)
    step = 512 if width % 512 == 0 else LANES
    for at in range(0, width, step):
        cols = slice(at, at + step)
        value = jnp.dot(hidden_a, down_a[0, :, cols], preferred_element_type=jnp.float32)
        value += jnp.dot(hidden_b, down_b[0, :, cols], preferred_element_type=jnp.float32)
        out[:, cols] = value * score


def expert_rows(rows, weights):
    count, width = rows.shape[0], weights[2].shape[2]
    tile = min(count, 256)
    return pl.pallas_call(
        expert_body,
        grid=(count // tile,),
        in_specs=[
            pl.BlockSpec((tile, rows.shape[1]), lambda i: (i, 0)),
        ]
        + [pl.BlockSpec(memory_space=pltpu.VMEM)] * len(weights),
        out_specs=pl.BlockSpec((tile, width), lambda i: (i, 0)),
        out_shape=jax.ShapeDtypeStruct((count, width), jnp.float32),
        compiler_params=pltpu.CompilerParams(
            dimension_semantics=("arbitrary",), vmem_limit_bytes=24 * 2**20
        ),
        name="experts",
    )(rows, *weights)


def shards(tokens, live_counts, expert_ids, gate_scores, gate_weight, up_weight, down_weight):
    count = lax.axis_size("expert")
    experts = count // 2
    own = (gate_weight, up_weight, down_weight)
    other = [swap(weight, (0, 0)) for weight in own]
    columns = routing_columns(live_counts, expert_ids, gate_scores, experts)
    rows = jnp.concatenate([tokens, columns], axis=1)
    stages = stage_bits(count)
    rows = gather_rows(rows, stages[:-2])
    own = lax.optimization_barrier((rows, own))[1]
    own = load_weights(own)
    rows = gather_rows(rows, stages[-2:-1])
    other = lax.optimization_barrier((rows, other))[1]
    other = load_weights(other)
    rows = gather_rows(rows, stages[-1:])
    part = expert_rows(rows, [*own, *other])
    return reduce_rows(part, count).astype(jnp.bfloat16)


def solution(mesh):
    in_specs = (
        P(("groups", "expert"), None),
        P(("groups", "expert")),
        P(("groups", "expert"), None),
        P(("groups", "expert"), None),
        P("expert", None, None),
        P("expert", None, None),
        P("expert", None, None),
    )
    out_specs = P(("groups", "expert"), None)
    return jax.shard_map(shards, mesh=mesh, in_specs=in_specs, out_specs=out_specs, check_vma=False)
```

```python
import jax
import jax.numpy as jnp
from jax import lax
from jax.experimental import pallas as pl
from jax.experimental.pallas import tpu as pltpu
from jax.sharding import PartitionSpec as P

LANES = 128


def stage_bits(count):
    top = count.bit_length() - 1
    even = list(range(top - 1, 0, -1))
    odd = even[-1:] + even[:-1]
    return list(zip(even, odd))


def swap(block, bits):
    count = lax.axis_size("expert")
    route = [(i, i ^ (1 << bits[i & 1])) for i in range(count)]
    return lax.ppermute(block, "expert", route)


def gather_rows(rows, stages):
    for bits in stages:
        rows = jnp.concatenate([rows, swap(rows, bits)], axis=0)
    return rows


def reduce_rows(part, count):
    for bits in stage_bits(count)[::-1]:
        half = part.shape[0] // 2
        got = swap(part[half:].astype(jnp.bfloat16), bits)
        part = part[:half] + got.astype(jnp.float32)
    return part


def routing_columns(live_counts, expert_ids, gate_scores, experts):
    slots = expert_ids.shape[0]
    live = jnp.arange(slots, dtype=jnp.int32)[:, None] < live_counts[0]
    named = expert_ids[:, :, None] == jnp.arange(experts, dtype=jnp.int32)
    score = jnp.sum(jnp.where(named & live[:, :, None], gate_scores[:, :, None], 0.0), axis=1)
    high = lax.reduce_precision(score, 8, 7)
    low = score - high
    pad = jnp.zeros((slots, -2 * experts % LANES), jnp.float32)
    return jnp.concatenate([high, low, pad], axis=1).astype(jnp.bfloat16)


def load_body(*refs):
    half = len(refs) // 2
    sources, targets, sems = refs[:half], refs[half:-1], refs[-1]
    copies = [
        pltpu.make_async_copy(source, target, sems.at[i])
        for i, (source, target) in enumerate(zip(sources, targets))
    ]
    for copy in copies:
        copy.start()
    for copy in copies:
        copy.wait()


def load_weights(weights):
    return pl.pallas_call(
        load_body,
        in_specs=[pl.BlockSpec(memory_space=pltpu.HBM)] * len(weights),
        out_specs=[pl.BlockSpec(memory_space=pltpu.VMEM)] * len(weights),
        out_shape=[pltpu.VMEM(w.shape, w.dtype) for w in weights],
        scratch_shapes=[pltpu.SemaphoreType.DMA((len(weights),))],
        cost_estimate=pl.CostEstimate(
            flops=10**10, bytes_accessed=0, transcendentals=0
        ),
        compiler_params=pltpu.CompilerParams(vmem_limit_bytes=2**20),
        name="load",
    )(*weights)


def expert_body(rows, gate_a, up_a, down_a, gate_b, up_b, down_b, out):
    width = out.shape[1]
    inputs = rows[:, :width]
    columns = rows[:, width:].astype(jnp.float32)
    experts = lax.axis_size("expert") // 2
    mine = lax.shift_right_logical(lax.axis_index("expert"), 1)
    lane = lax.broadcasted_iota(jnp.int32, columns.shape, 1)
    named = (lane == mine) | (lane == mine + experts)
    score = jnp.sum(jnp.where(named, columns, 0.0), axis=1, keepdims=True)

    def hidden(gate, up):
        gate_act = jnp.dot(inputs, gate[0], preferred_element_type=jnp.float32)
        up_act = jnp.dot(inputs, up[0], preferred_element_type=jnp.float32)
        return (gate_act / (1.0 + jnp.exp(-gate_act)) * up_act).astype(jnp.bfloat16)

    hidden_a, hidden_b = hidden(gate_a, up_a), hidden(gate_b, up_b)
    step = 512 if width % 512 == 0 else LANES
    for at in range(0, width, step):
        cols = slice(at, at + step)
        value = jnp.dot(hidden_a, down_a[0, :, cols], preferred_element_type=jnp.float32)
        value += jnp.dot(hidden_b, down_b[0, :, cols], preferred_element_type=jnp.float32)
        out[:, cols] = value * score


def expert_rows(rows, weights):
    count, width = rows.shape[0], weights[2].shape[2]
    tile = min(count, 256)
    return pl.pallas_call(
        expert_body,
        grid=(count // tile,),
        in_specs=[
            pl.BlockSpec((tile, rows.shape[1]), lambda i: (i, 0)),
        ]
        + [pl.BlockSpec(memory_space=pltpu.VMEM)] * len(weights),
        out_specs=pl.BlockSpec((tile, width), lambda i: (i, 0)),
        out_shape=jax.ShapeDtypeStruct((count, width), jnp.float32),
        compiler_params=pltpu.CompilerParams(
            dimension_semantics=("arbitrary",), vmem_limit_bytes=24 * 2**20
        ),
        name="experts",
    )(rows, *weights)


def shards(tokens, live_counts, expert_ids, gate_scores, gate_weight, up_weight, down_weight):
    count = lax.axis_size("expert")
    experts = count // 2
    own = (gate_weight, up_weight, down_weight)
    other = [swap(weight, (0, 0)) for weight in own]
    columns = routing_columns(live_counts, expert_ids, gate_scores, experts)
    rows = jnp.concatenate([tokens, columns], axis=1)
    stages = stage_bits(count)
    rows = gather_rows(rows, stages[:-2])
    rows, own = lax.optimization_barrier((rows, own))
    own = load_weights(own)
    rows = gather_rows(rows, stages[-2:-1])
    rows, other = lax.optimization_barrier((rows, other))
    other = load_weights(other)
    rows = gather_rows(rows, stages[-1:])
    part = expert_rows(rows, [*own, *other])
    return reduce_rows(part, count).astype(jnp.bfloat16)


def solution(mesh):
    in_specs = (
        P(("groups", "expert"), None),
        P(("groups", "expert")),
        P(("groups", "expert"), None),
        P(("groups", "expert"), None),
        P("expert", None, None),
        P("expert", None, None),
        P("expert", None, None),
    )
    out_specs = P(("groups", "expert"), None)
    return jax.shard_map(shards, mesh=mesh, in_specs=in_specs, out_specs=out_specs, check_vma=False)
```
